32 devices in a mesh: ctx: 8 (over z, x), head: 4 (over y, core).
Axes of the slice: x: 2, y: 2, z: 4, core: 2. Of those that a mesh axis runs over, the one named last changes fastest.
Arguments:
- queries: bfloat16 [256, 4096], P(None, 'head'), may hold values from -40 to 40
- keys: bfloat16 [16, 2048, 2048], P('ctx', None, 'head'), may hold values from -6 to 6
- values: bfloat16 [16, 2048, 2048], P('ctx', None, 'head'), may hold values from -6 to 6
- page_map: int32 [16], replicated, may hold values from 0 to 15, each once
- selected: int32 [2, 8], replicated, may hold values from 0 to 15, as said below
- residual_in: bfloat16 [256, 5376], P('head', 'ctx'), may hold values from -7 to 7
- out_weight: bfloat16 [4096, 5376], P('head', 'ctx'), may hold values from -0.09375 to 0.09375
- norm_gain: float32 [5376], P('ctx'), may hold values from 0.5 to 1.5
- gate_weight: bfloat16 [5376, 21504], P('head', 'ctx'), may hold values from -0.078125 to 0.078125
- up_weight: bfloat16 [5376, 21504], P('head', 'ctx'), may hold values from -0.078125 to 0.078125
- down_weight: bfloat16 [21504, 5376], P('ctx', 'head'), may hold values from -0.0390625 to 0.0390625
Outputs:
- layer_out: bfloat16 [256, 5376], P('ctx', 'head')
The draws below stay inside these ranges and needn't reach their ends.
Inputs may be any that keep to these rules, and one draw needn't show every extreme that they name: `selected`: each row names 8 different logical pages, among them 16 - 1, the page that holds the block's own positions.
All inputs are finite; a program needn't handle non-finite values.
Results may differ from the reference program's by a relative error of at most 0.02.
Values may be sent and summed in bfloat16 or wider, within the bound.
A program may use at most 128 MiB of HBM per device.

```python
import jax
import jax.numpy as jnp
from jax import lax

D = 5376
FF = 21504
QUERY_HEADS = 32
KEY_VALUE_HEADS = 16
HEAD_SIZE = 128
PAGE_TOKENS = 2048
TILE_QUERY_ROWS = 128
PAGES_PER_TILE = 8
TILES = 2
CACHE_PAGES = 16


def insert_vectors(key):
    sign_values = jax.random.bernoulli(jax.random.fold_in(key, 7), 0.5, (KEY_VALUE_HEADS, HEAD_SIZE))
    return jnp.where(sign_values, 1.0, -1.0).astype(jnp.float32)


def marked_slots(key):
    chosen = jax.random.bernoulli(jax.random.fold_in(key, 8), 0.5, (CACHE_PAGES,))
    return chosen.at[0].set(True)


def draw_queries(key, part):
    row_count = TILES * TILE_QUERY_ROWS
    base_vector = jnp.clip(3.0 * jax.random.normal(jax.random.fold_in(key, 1), (row_count, QUERY_HEADS * HEAD_SIZE), jnp.float32), -24.0, 24.0)
    vector_rows = insert_vectors(key)
    inserted_rows = jnp.repeat(vector_rows, QUERY_HEADS // KEY_VALUE_HEADS, axis=0).reshape(QUERY_HEADS * HEAD_SIZE)
    row_ids = jnp.arange(row_count)
    target = 130.0 + 50.0 * (row_ids // TILE_QUERY_ROWS % 3).astype(jnp.float32)
    strength = jnp.minimum(target * 168.0 ** 0.5 / (5.0 * HEAD_SIZE), 40.0)
    marked = row_ids % TILE_QUERY_ROWS == TILE_QUERY_ROWS // 2
    base_vector = jnp.where(marked[:, None], strength[:, None] * inserted_rows[None, :], base_vector)
    return base_vector.astype(jnp.bfloat16)


def draw_keys(key, part):
    base_vector = jnp.clip(jax.random.normal(jax.random.fold_in(key, 2), (CACHE_PAGES, PAGE_TOKENS, KEY_VALUE_HEADS * HEAD_SIZE), jnp.float32), -6.0, 6.0)
    vector_rows = 5.0 * insert_vectors(key).reshape(KEY_VALUE_HEADS * HEAD_SIZE)
    hot = marked_slots(key)[:, None]
    base_vector = base_vector.at[:, 0, :].set(jnp.where(hot, vector_rows[None, :], base_vector[:, 0, :]))
    base_vector = base_vector.at[:, 1, :].set(jnp.where(hot, 0.992 * vector_rows[None, :], base_vector[:, 1, :]))
    return base_vector.astype(jnp.bfloat16)


def draw_selected(key, part):
    popular = jax.random.randint(jax.random.fold_in(key, 3), (CACHE_PAGES,), 0, 4)
    jitter = jax.random.randint(jax.random.fold_in(key, 4), (TILES, CACHE_PAGES), 0, 64)
    page_ids = jnp.arange(CACHE_PAGES, dtype=jnp.int32)
    ranking = (popular[None, :] * 64 + jitter) * CACHE_PAGES + page_ids[None, :]
    ranking = jnp.where(page_ids[None, :] == CACHE_PAGES - 1, 1 << 29, ranking)
    picked = lax.top_k(ranking, PAGES_PER_TILE)[1]
    return picked.astype(jnp.int32)


def draw_residual_in(key, part):
    row_count = TILES * TILE_QUERY_ROWS
    row_scale = jnp.exp(jax.random.uniform(jax.random.fold_in(key, 5), (row_count, 1), jnp.float32, -0.69, 0.4))
    column = jnp.arange(D).astype(jnp.float32) / D
    column_scale = 0.5 * 3.0 ** column
    base_vector = jnp.clip(jax.random.normal(jax.random.fold_in(key, 6), (row_count, D), jnp.float32), -3.0, 3.0)
    return (base_vector * row_scale * column_scale[None, :]).astype(jnp.bfloat16)


def levels(own_key, extent, cuts, least, top_value):
    def one(dim, blocks):
        heights = jax.random.uniform(jax.random.fold_in(jax.random.fold_in(own_key, 6), dim), (blocks,), jnp.float32, least / len(cuts), top_value / len(cuts))
        return jnp.repeat(jnp.exp(heights), extent[dim] // blocks).reshape((-1,) + (1,) * (len(extent) - dim - 1))

    gain = one(*cuts[0])
    for cut in cuts[1:]:
        gain = gain * one(*cut)
    return gain


def gaussian(stream_key, extent, width, reach, split=(), kind=jnp.bfloat16):
    entries = width * jax.random.normal(stream_key, extent, jnp.float32)
    if split:
        entries = entries * levels(stream_key, extent, split, -0.22, 0.18)
    return jnp.clip(entries, -reach, reach).astype(kind)


def setup_inputs(seed: int = 0) -> dict:
    splits = jax.random.split(jax.random.key(seed), 12)
    queries = draw_queries(jax.random.fold_in(splits[11], 71), 0)
    keys = draw_keys(jax.random.fold_in(splits[11], 71), 0)
    values = gaussian(splits[2], (CACHE_PAGES, PAGE_TOKENS, KEY_VALUE_HEADS * HEAD_SIZE), 1.0, 6.0, ((0, 8), (2, 4)))
    page_map = jax.random.permutation(splits[3], CACHE_PAGES).astype(jnp.int32)
    selected = draw_selected(jax.random.fold_in(splits[11], 71), 0)
    residual_in = draw_residual_in(jax.random.fold_in(splits[11], 71), 0)
    out_weight = gaussian(splits[6], (QUERY_HEADS * HEAD_SIZE, D), (QUERY_HEADS * HEAD_SIZE) ** -0.5, 0.09375, ((0, 4), (1, 8)))
    norm_gain = jnp.clip(0.5 + 1.0 * jax.random.uniform(splits[7], (D,), jnp.float32) ** levels(splits[7], (D,), ((0, 8),), -0.2, 0.2), 0.5, 1.5)
    gate_weight = gaussian(splits[8], (D, FF), D ** -0.5, 0.078125, ((0, 4), (1, 8)))
    up_weight = gaussian(splits[9], (D, FF), D ** -0.5, 0.078125, ((0, 4), (1, 8)))
    down_weight = gaussian(splits[10], (FF, D), FF ** -0.5, 0.0390625, ((0, 8), (1, 4)))
    return dict(queries=queries, keys=keys, values=values, page_map=page_map, selected=selected, residual_in=residual_in, out_weight=out_weight, norm_gain=norm_gain, gate_weight=gate_weight, up_weight=up_weight, down_weight=down_weight)


score_scale = 168.0 ** (-0.5)
masked_score = -1e+30
norm_epsilon = 1e-06

def reference(queries, keys, values, page_map, selected, residual_in, out_weight, norm_gain, gate_weight, up_weight, down_weight):
    row_count = TILES * TILE_QUERY_ROWS
    offset = PAGE_TOKENS - row_count
    query_group_size = QUERY_HEADS // KEY_VALUE_HEADS
    slot_ids = jnp.take(page_map, selected, axis=0).astype(jnp.int32)
    is_causal = selected == CACHE_PAGES - 1
    key_position = jnp.arange(PAGE_TOKENS, dtype=jnp.int32)

    def one_tile(inputs):
        tile_query_rows, tile_page_slots, tile_causal, tile_index = inputs
        tile_key_rows = jnp.take(keys, tile_page_slots, axis=0).reshape(PAGES_PER_TILE * PAGE_TOKENS, KEY_VALUE_HEADS, HEAD_SIZE).astype(jnp.float32)
        tile_value_rows = jnp.take(values, tile_page_slots, axis=0).reshape(PAGES_PER_TILE * PAGE_TOKENS, KEY_VALUE_HEADS, HEAD_SIZE).astype(jnp.float32)
        grouped_queries = tile_query_rows.reshape(TILE_QUERY_ROWS, KEY_VALUE_HEADS, query_group_size, HEAD_SIZE).astype(jnp.float32)
        scores = jnp.einsum('qkgd,jkd->kgqj', grouped_queries, tile_key_rows) * score_scale
        query_position = offset + tile_index * TILE_QUERY_ROWS + jnp.arange(TILE_QUERY_ROWS, dtype=jnp.int32)
        visible = jnp.logical_or(jnp.logical_not(tile_causal)[:, None, None], key_position[None, None, :] <= query_position[None, :, None])
        visible = jnp.transpose(visible, (1, 0, 2)).reshape(TILE_QUERY_ROWS, PAGES_PER_TILE * PAGE_TOKENS)
        scores = jnp.where(visible[None, None], scores, masked_score)
        row_max = lax.optimization_barrier(jnp.max(scores, axis=-1, keepdims=True))
        weights = jnp.where(visible[None, None], jnp.exp(scores - row_max), 0.0)
        row_total = lax.optimization_barrier(jnp.sum(weights, axis=-1))
        rounded = lax.optimization_barrier(weights.astype(jnp.bfloat16)).astype(jnp.float32)
        mixture = jnp.einsum('kgqj,jkd->qkgd', rounded, tile_value_rows)
        mixture = mixture / jnp.transpose(row_total, (2, 0, 1))[..., None]
        return mixture.reshape(TILE_QUERY_ROWS, QUERY_HEADS * HEAD_SIZE).astype(jnp.bfloat16)
    tiled = queries.reshape(TILES, TILE_QUERY_ROWS, QUERY_HEADS * HEAD_SIZE)
    attention = lax.map(one_tile, (tiled, slot_ids, is_causal, jnp.arange(TILES, dtype=jnp.int32)))
    attention = attention.reshape(row_count, QUERY_HEADS * HEAD_SIZE)
    projected = jnp.dot(attention, out_weight, preferred_element_type=jnp.float32)
    stream = (residual_in.astype(jnp.float32) + projected).astype(jnp.bfloat16)
    stream_float = stream.astype(jnp.float32)
    mean_square = lax.optimization_barrier(jnp.mean(stream_float * stream_float, axis=-1, keepdims=True))
    normed = (stream_float * lax.rsqrt(mean_square + norm_epsilon) * norm_gain).astype(jnp.bfloat16)
    gate = jnp.dot(normed, gate_weight, preferred_element_type=jnp.float32)
    upward = jnp.dot(normed, up_weight, preferred_element_type=jnp.float32)
    hidden = (jax.nn.gelu(gate, approximate=True) * upward).astype(jnp.bfloat16)
    mlp_out = jnp.dot(hidden, down_weight, preferred_element_type=jnp.float32)
    return (stream_float + mlp_out).astype(jnp.bfloat16)
```

```python
import jax
import jax.numpy as jnp
import functools
from jax import lax
from jax.experimental import pallas as pl
from jax.experimental.pallas import tpu as pltpu
from jax.sharding import PartitionSpec as P

D = 5376
HEAD_SIZE = 128


score_scale = 168.0 ** (-0.5)
masked_score = -1e30
norm_epsilon = 1e-06


def block_scores(grouped_queries, block_keys, block_values, visible):
    scores = (
        jnp.einsum(
            "rkgd,jkd->kgrj", grouped_queries, block_keys, preferred_element_type=jnp.float32
        )
        * score_scale
    )
    scores = jnp.where(visible[None, None], scores, masked_score)
    row_max = jnp.max(scores, axis=-1)
    weights = jnp.where(visible[None, None], jnp.exp(scores - row_max[..., None]), 0.0)
    row_total = jnp.sum(weights, axis=-1)
    mixture = jnp.einsum(
        "kgrj,jkd->rkgd",
        weights.astype(jnp.bfloat16),
        block_values,
        preferred_element_type=jnp.float32,
    )
    row_count = grouped_queries.shape[0]
    row_max = jnp.transpose(row_max, (2, 0, 1)).reshape(row_count, -1)
    row_total = jnp.transpose(row_total, (2, 0, 1)).reshape(row_count, -1)
    return (row_max, row_total, mixture.reshape(row_count, -1))


def merge_parts(earlier, later):
    new_max = jnp.maximum(earlier[0], later[0])
    earlier_scale = jnp.exp(earlier[0] - new_max)
    later_scale = jnp.exp(later[0] - new_max)
    row_total = earlier[1] * earlier_scale + later[1] * later_scale
    row_count, head_count = new_max.shape
    mixture = earlier[2].reshape(row_count, head_count, -1) * earlier_scale[..., None]
    mixture = mixture + later[2].reshape(row_count, head_count, -1) * later_scale[..., None]
    return (new_max, row_total, mixture.reshape(row_count, -1))


def owner_pass(queries, keys, values, page_map, selected, ctx_index, ctx_count):
    pages_local, page_len, kv_width = keys.shape
    row_count, query_width = queries.shape
    kv_local = kv_width // HEAD_SIZE
    query_group_size = query_width // kv_width
    heads_local = kv_local * query_group_size
    tile_count = selected.shape[0]
    tile_rows = row_count // tile_count
    page_total = pages_local * ctx_count
    offset = page_len - row_count
    slot_ids = ctx_index * pages_local + jnp.arange(pages_local, dtype=jnp.int32)
    all_pages = jnp.arange(page_total, dtype=jnp.int32)
    logical = jnp.sum(
        jnp.where(page_map[None, :] == slot_ids[:, None], all_pages[None, :], 0), axis=1
    )
    chosen = jnp.any(selected[:, None, :] == logical[None, :, None], axis=2)
    is_causal = logical == page_total - 1
    key_position = jnp.arange(page_len, dtype=jnp.int32)
    grouped_tiles = queries.reshape(tile_count, tile_rows, kv_local, query_group_size, HEAD_SIZE)
    page_keys = keys.reshape(pages_local, page_len, kv_local, HEAD_SIZE)
    page_values = values.reshape(pages_local, page_len, kv_local, HEAD_SIZE)

    def one_tile(inputs):
        grouped_queries, tile_index, tile_chosen = inputs
        query_position = offset + tile_index * tile_rows + jnp.arange(tile_rows, dtype=jnp.int32)
        result = (
            jnp.full((tile_rows, heads_local), masked_score, jnp.float32),
            jnp.zeros((tile_rows, heads_local), jnp.float32),
            jnp.zeros((tile_rows, heads_local * HEAD_SIZE), jnp.float32),
        )
        for page_index in range(pages_local):
            visible = jnp.logical_or(
                jnp.logical_not(is_causal[page_index]),
                key_position[None, :] <= query_position[:, None],
            )

            def compute(carry, page_index=page_index, visible=visible):
                return merge_parts(
                    carry,
                    block_scores(
                        grouped_queries, page_keys[page_index], page_values[page_index], visible
                    ),
                )

            def keep(carry):
                return carry

            result = lax.cond(tile_chosen[page_index], compute, keep, result)
        return result

    tiles_out = lax.map(one_tile, (grouped_tiles, jnp.arange(tile_count, dtype=jnp.int32), chosen))
    return tuple((stacked.reshape(row_count, -1) for stacked in tiles_out))


MESH = pl.DeviceIdType.MESH
CORES = 2


def column_tile(width):
    for tile in (896, 768, 640, 512, 384, 256, 128):
        if width % tile == 0:
            return tile
    return width


def flat(block, rows):
    if block.shape[1] % 16:
        return block.astype(jnp.float32).reshape(rows, -1).astype(jnp.bfloat16)
    return block.reshape(rows, -1)


def tail_kernel(
    C,
    H,
    mix_ref,
    stat_ref,
    res_ref,
    gain_ref,
    ow_hbm,
    gw_hbm,
    uw_hbm,
    dw_hbm,
    mlp_ref,
    own_ref,
    ow,
    gw,
    uw,
    dw,
    mix_in,
    stat_in,
    att,
    po,
    po_in,
    u_out,
    st_out,
    ss,
    ublk,
    own_st,
    first,
    first_in,
    second,
    second_in,
    hid,
    acc,
    part,
    part_in,
    w_sem,
    mix_s,
    mix_r,
    stat_s,
    stat_r,
    att_s,
    att_r,
    po_s,
    po_r,
    u_s,
    u_r,
    st_s,
    st_r,
    ss_s,
    ss_r,
    f_s,
    f_r,
    g_s,
    g_r,
    h_s,
    h_r,
    fw_s,
    part_s,
    part_r,
):
    c = lax.axis_index("ctx")
    h = lax.axis_index("head")
    Y = H // CORES
    y = h // CORES
    core = h % CORES
    partner = y * CORES + (CORES - 1 - core)
    R = mix_ref.shape[1]
    rows = C * R
    rb = C // H
    bph = C // H
    width = ow.shape[1]
    head_rows = rows // H
    heads = mix_ref.shape[2] // HEAD_SIZE
    tiles, _, _, _, _, tile = first.shape
    f32 = jnp.float32
    bf16 = jnp.bfloat16

    def remote(src, dst, send_sem, recv_sem, ctx, head):
        return pltpu.make_async_remote_copy(
            src_ref=src,
            dst_ref=dst,
            send_sem=send_sem,
            recv_sem=recv_sem,
            device_id=(ctx, head),
            device_id_type=MESH,
        )

    sent = []

    def send(*args):
        copy = remote(*args)
        copy.start()
        sent.append(copy)

    loads = [
        pltpu.make_async_copy(src, dst, w_sem.at[i])
        for i, (src, dst) in enumerate(
            ((ow_hbm, ow), (gw_hbm, gw), (uw_hbm, uw), (dw_hbm, dw))
        )
    ]
    for load in loads:
        load.start()

    for d in range(1, C):
        peer = (c + d) % C
        send(stat_ref.at[peer], stat_in.at[c], stat_s.at[d], stat_r.at[c], peer, h)
        send(mix_ref.at[peer], mix_in.at[c], mix_s.at[d], mix_r.at[c], peer, h)
    stat_in[c] = stat_ref[c]
    mix_in[c] = mix_ref[c]
    for d in range(1, C):
        peer = (c + C - d) % C
        remote(stat_in.at[peer], stat_in.at[peer], stat_s.at[d], stat_r.at[peer], peer, h).wait_recv()
        remote(mix_in.at[peer], mix_in.at[peer], mix_s.at[d], mix_r.at[peer], peer, h).wait_recv()
    maxima = [stat_in[k][:, :heads] for k in range(C)]
    top = functools.reduce(jnp.maximum, maxima)
    scales = [jnp.exp(m - top) for m in maxima]
    total = sum(stat_in[k][:, heads : 2 * heads] * scales[k] for k in range(C))
    inverse = 1.0 / total
    for g in range(heads):
        cols = slice(g * HEAD_SIZE, (g + 1) * HEAD_SIZE)
        mixed = sum(mix_in[k, :, cols].astype(f32) * scales[k][:, g : g + 1] for k in range(C))
        att[c, :, cols] = (mixed * inverse[:, g : g + 1]).astype(bf16)

    for d in range(1, C):
        peer = (c + d) % C
        send(att.at[c], att.at[c], att_s.at[d], att_r.at[c], peer, h)
    loads[0].wait()
    for d in range(1, C):
        peer = (c + C - d) % C
        remote(att.at[peer], att.at[peer], att_s.at[d], att_r.at[peer], peer, h).wait_recv()
    projected = jnp.dot(flat(att[...], rows), ow[...], preferred_element_type=f32)
    po[...] = projected.reshape(H, head_rows, width).astype(bf16)

    for d in range(1, H):
        peer = (h + d) % H
        send(po.at[peer], po_in.at[h], po_s.at[d], po_r.at[h], c, peer)
    po_in[h] = po[h]
    for d in range(1, H):
        peer = (h + H - d) % H
        remote(po_in.at[peer], po_in.at[peer], po_s.at[d], po_r.at[peer], c, peer).wait_recv()
    projected = sum(po_in[k].astype(f32) for k in range(H))
    stream = (res_ref[...].astype(f32) + projected).astype(bf16).astype(f32)
    st_out[...] = stream.reshape(rb, R, width).astype(bf16)
    u_out[...] = (stream * gain_ref[...]).reshape(rb, R, width).astype(bf16)
    squares = jnp.sum(stream * stream, axis=1, keepdims=True)
    ss[c] = jnp.broadcast_to(squares, (head_rows, 128))

    block_head = c // bph
    block_part = c % bph
    u_dst = ublk.at[block_part, pl.ds(h * rb, rb)]
    kept = []
    for d in range(C):
        peer = (c + d) % C
        copy = remote(u_out, u_dst, u_s.at[d], u_r.at[block_part, h], peer, block_head)
        if d == 0:
            kept.append((block_head != h, copy))
            pl.when(block_head != h)(copy.start)

            @pl.when(block_head == h)
            def _():
                ublk[block_part, pl.ds(h * rb, rb)] = u_out[...]

        else:
            copy.start()
            sent.append(copy)
    for d in range(1, C):
        peer = (c + d) % C
        send(ss.at[c], ss.at[c], ss_s.at[d], ss_r.at[c], peer, h)
    for i in range(rb):
        owner = h * rb + i
        other = jnp.logical_or(owner != c, block_head != h)
        copy = remote(
            st_out.at[i], own_st.at[block_part], st_s.at[i], st_r.at[block_part], owner, block_head
        )
        kept.append((other, copy))
        pl.when(other)(copy.start)

        @pl.when(jnp.logical_not(other))
        def _(i=i):
            own_st[block_part] = st_out[i]

    for j in range(bph):
        for k in range(H):
            source = h * bph + j
            block = ublk.at[j, pl.ds(k * rb, rb)]
            arrival = remote(block, block, u_s.at[0], u_r.at[j, k], source, k)
            pl.when(jnp.logical_or(source != c, h != k))(arrival.wait_recv)
    loads[1].wait()
    loads[2].wait()

    def matmul(i, which, weight):
        cols = slice(i * tile, (i + 1) * tile)
        value = None
        for j in range(bph):
            term = jnp.dot(
                flat(ublk[j], rows),
                weight[j * width : (j + 1) * width, cols],
                preferred_element_type=f32,
            )
            value = term if value is None else value + term
        first[i, which] = value.reshape(Y, CORES, head_rows, tile).swapaxes(0, 1).astype(bf16)
        send(
            first.at[i, which, CORES - 1 - core],
            first_in.at[i, which],
            f_s.at[i, which],
            f_r.at[i, which],
            c,
            partner,
        )

    def middle(i, which):
        remote(
            first_in.at[i, which], first_in.at[i, which], f_s.at[i, which], f_r.at[i, which], c, partner
        ).wait_recv()
        both = first[i, which, core].astype(f32) + first_in[i, which].astype(f32)
        second[i, which] = both.astype(bf16)
        for d in range(1, Y):
            peer = (y + d) % Y
            send(
                second.at[i, which, peer],
                second_in.at[i, which, y],
                g_s.at[i, which, d],
                g_r.at[i, which, y],
                c,
                peer * CORES + core,
            )

    def finish(i, inverse_rms):
        sums = []
        for which in range(2):
            value = second[i, which, y].astype(f32)
            for d in range(1, Y):
                peer = (y + Y - d) % Y
                slot = second_in.at[i, which, peer]
                remote(
                    slot, slot, g_s.at[i, which, d], g_r.at[i, which, peer], c, peer * CORES + core
                ).wait_recv()
                value = value + second_in[i, which, peer].astype(f32)
            sums.append(value * inverse_rms)
        hid[i, h] = (jax.nn.gelu(sums[0], approximate=True) * sums[1]).astype(bf16)
        send(hid.at[i, h], hid.at[i, h], h_s.at[i, 0], h_r.at[i, h], c, partner)
        for d in range(1, Y):
            peer = ((y + d) % Y) * CORES + core
            send(hid.at[i, h], hid.at[i, h], h_s.at[i, d], h_r.at[i, h], c, peer)

    def forward(i):
        for d in range(1, Y):
            origin = ((y + Y - d) % Y) * CORES + core
            slot = hid.at[i, origin]
            remote(slot, slot, h_s.at[i, d], h_r.at[i, origin], c, origin).wait_recv()
            send(slot, slot, fw_s.at[i, d], h_r.at[i, origin], c, partner)

    def down(i):
        for d in range(Y):
            origin = ((y + Y - d) % Y) * CORES + (CORES - 1 - core)
            slot = hid.at[i, origin]
            remote(slot, slot, h_s.at[i, 0], h_r.at[i, origin], c, partner).wait_recv()
        term = jnp.dot(
            flat(hid[i], rows), dw[i * tile : (i + 1) * tile, :], preferred_element_type=f32
        )
        if i == 0:
            acc[...] = term
        else:
            acc[...] += term

    steps = [(i, which) for i in range(tiles) for which in range(2)]
    for n, (i, which) in enumerate(steps):
        matmul(i, which, (gw, uw)[which])
        if n:
            middle(*steps[n - 1])
    middle(*steps[-1])
    for d in range(1, C):
        peer = (c + C - d) % C
        remote(ss.at[peer], ss.at[peer], ss_s.at[d], ss_r.at[peer], peer, h).wait_recv()
    squares = sum(ss[k] for k in range(C))
    inverse_rms = lax.rsqrt(squares[:, :1] / (C * width) + norm_epsilon)
    loads[3].wait()
    for i in range(tiles):
        finish(i, inverse_rms)
        if i:
            forward(i - 1)
    forward(tiles - 1)
    for i in range(tiles):
        down(i)
    part[...] = acc[...].reshape(C, R, acc.shape[1]).astype(bf16)

    for d in range(1, C):
        peer = (c + d) % C
        send(part.at[peer], part_in.at[c], part_s.at[d], part_r.at[c], peer, h)
    part_in[c] = part[c]
    for j in range(bph):
        source = h * bph + j
        arrival = remote(own_st.at[j], own_st.at[j], st_s.at[0], st_r.at[j], source, c // rb)
        pl.when(jnp.logical_or(source != c, c // rb != h))(arrival.wait_recv)
    own_ref[...] = own_st[...]
    for d in range(1, C):
        peer = (c + C - d) % C
        remote(part_in.at[peer], part_in.at[peer], part_s.at[d], part_r.at[peer], peer, h).wait_recv()
    mlp_ref[...] = sum(part_in[k].astype(f32) for k in range(C))
    for copy in sent:
        copy.wait_send()
    for condition, copy in kept:
        pl.when(condition)(copy.wait_send)


def tail(C, H, mixture, stats, residual_in, norm_gain, out_weight, gate_weight, up_weight, down_weight):
    rows, query_width = mixture.shape
    R = rows // C
    width = out_weight.shape[1]
    hidden = gate_weight.shape[1]
    out_width = down_weight.shape[1]
    rb = C // H
    bph = C // H
    Y = H // CORES
    head_rows = rows // H
    tile = column_tile(hidden)
    tiles = hidden // tile
    bf16 = jnp.bfloat16
    vmem = pl.BlockSpec(memory_space=pltpu.VMEM)
    hbm = pl.BlockSpec(memory_space=pl.ANY)
    V = pltpu.VMEM
    S = pltpu.SemaphoreType.DMA
    return pl.pallas_call(
        functools.partial(tail_kernel, C, H),
        out_shape=(
            jax.ShapeDtypeStruct((R, out_width), jnp.float32),
            jax.ShapeDtypeStruct((bph, R, width), bf16),
        ),
        in_specs=[vmem] * 4 + [hbm] * 4,
        out_specs=(vmem, vmem),
        scratch_shapes=[
            V(out_weight.shape, bf16),
            V(gate_weight.shape, bf16),
            V(up_weight.shape, bf16),
            V(down_weight.shape, bf16),
            V((C, R, query_width), bf16),
            V((C, R, 128), jnp.float32),
            V((C, R, query_width), bf16),
            V((H, head_rows, width), bf16),
            V((H, head_rows, width), bf16),
            V((rb, R, width), bf16),
            V((rb, R, width), bf16),
            V((C, head_rows, 128), jnp.float32),
            V((bph, C, R, width), bf16),
            V((bph, R, width), bf16),
            V((tiles, 2, CORES, Y, head_rows, tile), bf16),
            V((tiles, 2, Y, head_rows, tile), bf16),
            V((tiles, 2, Y, head_rows, tile), bf16),
            V((tiles, 2, Y, head_rows, tile), bf16),
            V((tiles, H, head_rows, tile), bf16),
            V((rows, out_width), jnp.float32),
            V((C, R, out_width), bf16),
            V((C, R, out_width), bf16),
            S((4,)),
            S((C,)),
            S((C,)),
            S((C,)),
            S((C,)),
            S((C,)),
            S((C,)),
            S((H,)),
            S((H,)),
            S((C,)),
            S((bph, H)),
            S((rb,)),
            S((bph,)),
            S((C,)),
            S((C,)),
            S((tiles, 2)),
            S((tiles, 2)),
            S((tiles, 2, Y)),
            S((tiles, 2, Y)),
            S((tiles, Y)),
            S((tiles, H)),
            S((tiles, Y)),
            S((C,)),
            S((C,)),
        ],
        compiler_params=pltpu.CompilerParams(
            has_side_effects=True, vmem_limit_bytes=60 * 2**20
        ),
    )(
        mixture.reshape(C, R, query_width),
        stats.reshape(C, R, 128),
        residual_in,
        norm_gain.reshape(1, width),
        out_weight,
        gate_weight,
        up_weight,
        down_weight,
    )


def shards(
    queries,
    keys,
    values,
    page_map,
    selected,
    residual_in,
    out_weight,
    norm_gain,
    gate_weight,
    up_weight,
    down_weight,
):
    ctx_index = lax.axis_index("ctx")
    C = lax.axis_size("ctx")
    H = lax.axis_size("head")
    row_max, row_total, mixture = owner_pass(
        queries, keys, values, page_map, selected, ctx_index, C
    )
    stats = jnp.concatenate([row_max, row_total], axis=1)
    stats = jnp.pad(stats, ((0, 0), (0, 128 - stats.shape[1])))
    mlp_out, own_stream = tail(
        C,
        H,
        mixture.astype(jnp.bfloat16),
        stats,
        residual_in,
        norm_gain,
        out_weight,
        gate_weight,
        up_weight,
        down_weight,
    )
    own_stream = jnp.concatenate([own_stream[j] for j in range(own_stream.shape[0])], axis=1)
    return (own_stream.astype(jnp.float32) + mlp_out).astype(jnp.bfloat16)


def solution(mesh):
    in_specs = (
        P(None, "head"),
        P("ctx", None, "head"),
        P("ctx", None, "head"),
        P(),
        P(),
        P("head", "ctx"),
        P("head", "ctx"),
        P("ctx"),
        P("head", "ctx"),
        P("head", "ctx"),
        P("ctx", "head"),
    )
    out_specs = P("ctx", "head")
    return jax.shard_map(shards, mesh=mesh, in_specs=in_specs, out_specs=out_specs, check_vma=False)
```

```python
import jax
import jax.numpy as jnp
import functools
from jax import lax
from jax.experimental import pallas as pl
from jax.experimental.pallas import tpu as pltpu
from jax.sharding import PartitionSpec as P

D = 5376
HEAD_SIZE = 128


score_scale = 168.0 ** (-0.5)
masked_score = -1e30
norm_epsilon = 1e-06


def attention_kernel(
    logical_ref, chosen_ref, page_total, q_ref, k_ref, v_ref, mix_ref, m_ref, l_ref, acc, top, total
):
    page = pl.program_id(1)
    tile_count = chosen_ref.shape[0]
    tile_rows = q_ref.shape[0] // tile_count
    group = q_ref.shape[1] // k_ref.shape[2]
    page_len = k_ref.shape[1]
    offset = page_len - q_ref.shape[0]
    f32 = jnp.float32

    @pl.when(page == 0)
    def _():
        acc[...] = jnp.zeros_like(acc)
        top[...] = jnp.full_like(top, masked_score)
        total[...] = jnp.zeros_like(total)

    causal = logical_ref[page] == page_total - 1

    def visit(t, masked):
        rows = slice(t * tile_rows, (t + 1) * tile_rows)
        for g in range(group):
            cols = slice(g * HEAD_SIZE, (g + 1) * HEAD_SIZE)
            scores = (
                lax.dot_general(
                    q_ref[rows, cols],
                    k_ref[0],
                    (((1,), (1,)), ((), ())),
                    preferred_element_type=f32,
                )
                * score_scale
            )
            if masked:
                position = offset + t * tile_rows + lax.broadcasted_iota(jnp.int32, scores.shape, 0)
                key = lax.broadcasted_iota(jnp.int32, scores.shape, 1)
                scores = jnp.where(key <= position, scores, masked_score)
            old = top[g, rows, :1]
            new = jnp.maximum(old, jnp.max(scores, axis=1, keepdims=True))
            weights = jnp.exp(scores - new)
            keep = jnp.exp(old - new)
            total[g, rows] = total[g, rows] * keep + jnp.sum(weights, axis=1, keepdims=True)
            top[g, rows] = jnp.broadcast_to(new, (tile_rows, 128))
            acc[rows, cols] = acc[rows, cols] * keep + jnp.dot(
                weights.astype(jnp.bfloat16), v_ref[0], preferred_element_type=f32
            )

    for t in range(tile_count):
        picked = chosen_ref[t, page] != 0
        pl.when(jnp.logical_and(picked, causal))(functools.partial(visit, t, True))
        pl.when(jnp.logical_and(picked, jnp.logical_not(causal)))(
            functools.partial(visit, t, False)
        )

    @pl.when(page == pl.num_programs(1) - 1)
    def _():
        mix_ref[...] = acc[...].astype(jnp.bfloat16)
        lane = lax.broadcasted_iota(jnp.int32, m_ref.shape[1:], 1)
        maxima = jnp.zeros(m_ref.shape[1:], f32)
        sums = jnp.zeros(m_ref.shape[1:], f32)
        for g in range(group):
            maxima = jnp.where(lane == g, top[g], maxima)
            sums = jnp.where(lane == g, total[g], sums)
        m_ref[0] = maxima
        l_ref[0] = sums


def owner_pass(queries, keys, values, page_map, selected, ctx_index, ctx_count):
    pages_local, page_len, kv_width = keys.shape
    row_count, query_width = queries.shape
    kv_local = kv_width // HEAD_SIZE
    group = query_width // kv_width
    tile_count = selected.shape[0]
    page_total = pages_local * ctx_count
    slot_ids = ctx_index * pages_local + jnp.arange(pages_local, dtype=jnp.int32)
    all_pages = jnp.arange(page_total, dtype=jnp.int32)
    logical = jnp.sum(
        jnp.where(page_map[None, :] == slot_ids[:, None], all_pages[None, :], 0), axis=1
    )
    chosen = jnp.any(selected[:, None, :] == logical[None, :, None], axis=2).astype(jnp.int32)
    stat = jax.ShapeDtypeStruct((kv_local, row_count, 128), jnp.float32)
    stat_spec = pl.BlockSpec((1, row_count, 128), lambda k, p, a, b: (k, 0, 0))
    kv_spec = pl.BlockSpec((1, page_len, HEAD_SIZE), lambda k, p, a, b: (p, 0, k))
    q_spec = pl.BlockSpec((row_count, group * HEAD_SIZE), lambda k, p, a, b: (0, k))

    def kernel(logical_ref, chosen_ref, *refs):
        attention_kernel(logical_ref, chosen_ref, page_total, *refs)

    mixture, top, total = pl.pallas_call(
        kernel,
        grid_spec=pltpu.PrefetchScalarGridSpec(
            num_scalar_prefetch=2,
            grid=(kv_local, pages_local),
            in_specs=[q_spec, kv_spec, kv_spec],
            out_specs=(q_spec, stat_spec, stat_spec),
            scratch_shapes=[
                pltpu.VMEM((row_count, group * HEAD_SIZE), jnp.float32),
                pltpu.VMEM((group, row_count, 128), jnp.float32),
                pltpu.VMEM((group, row_count, 128), jnp.float32),
            ],
        ),
        out_shape=(jax.ShapeDtypeStruct((row_count, query_width), jnp.bfloat16), stat, stat),
    )(logical.astype(jnp.int32), chosen, queries, keys, values)

    def heads(stacked):
        return stacked[:, :, :group].transpose(1, 0, 2).reshape(row_count, kv_local * group)

    return heads(top), heads(total), mixture


MESH = pl.DeviceIdType.MESH
CORES = 2


def column_tile(width):
    for tile in (896, 768, 640, 512, 384, 256, 128):
        if width % tile == 0:
            return tile
    return width


def flat(block, rows):
    if block.shape[1] % 16:
        return block.astype(jnp.float32).reshape(rows, -1).astype(jnp.bfloat16)
    return block.reshape(rows, -1)


def tail_kernel(
    C,
    H,
    mix_ref,
    stat_ref,
    res_ref,
    gain_ref,
    ow_hbm,
    gw_hbm,
    uw_hbm,
    dw_hbm,
    mlp_ref,
    own_ref,
    ow,
    gw,
    uw,
    dw,
    mix_in,
    stat_in,
    att,
    po,
    po_in,
    u_out,
    st_out,
    ss,
    ublk,
    own_st,
    first,
    first_in,
    second,
    second_in,
    hid,
    acc,
    part,
    part_in,
    w_sem,
    mix_s,
    mix_r,
    stat_s,
    stat_r,
    att_s,
    att_r,
    po_s,
    po_r,
    u_s,
    u_r,
    st_s,
    st_r,
    ss_s,
    ss_r,
    f_s,
    f_r,
    g_s,
    g_r,
    h_s,
    h_r,
    fw_s,
    part_s,
    part_r,
):
    c = lax.axis_index("ctx")
    h = lax.axis_index("head")
    Y = H // CORES
    y = h // CORES
    core = h % CORES
    partner = y * CORES + (CORES - 1 - core)
    R = mix_ref.shape[1]
    rows = C * R
    rb = C // H
    bph = C // H
    width = ow.shape[1]
    head_rows = rows // H
    heads = mix_ref.shape[2] // HEAD_SIZE
    tiles, _, _, _, _, tile = first.shape
    f32 = jnp.float32
    bf16 = jnp.bfloat16

    def remote(src, dst, send_sem, recv_sem, ctx, head):
        return pltpu.make_async_remote_copy(
            src_ref=src,
            dst_ref=dst,
            send_sem=send_sem,
            recv_sem=recv_sem,
            device_id=(ctx, head),
            device_id_type=MESH,
        )

    sent = []

    def send(*args):
        copy = remote(*args)
        copy.start()
        sent.append(copy)

    loads = [
        pltpu.make_async_copy(src, dst, w_sem.at[i])
        for i, (src, dst) in enumerate(
            ((ow_hbm, ow), (gw_hbm, gw), (uw_hbm, uw), (dw_hbm, dw))
        )
    ]
    for load in loads:
        load.start()

    for d in range(1, C):
        peer = (c + d) % C
        send(stat_ref.at[peer], stat_in.at[c], stat_s.at[d], stat_r.at[c], peer, h)
        send(mix_ref.at[peer], mix_in.at[c], mix_s.at[d], mix_r.at[c], peer, h)
    stat_in[c] = stat_ref[c]
    mix_in[c] = mix_ref[c]
    for d in range(1, C):
        peer = (c + C - d) % C
        remote(stat_in.at[peer], stat_in.at[peer], stat_s.at[d], stat_r.at[peer], peer, h).wait_recv()
        remote(mix_in.at[peer], mix_in.at[peer], mix_s.at[d], mix_r.at[peer], peer, h).wait_recv()
    maxima = [stat_in[k][:, :heads] for k in range(C)]
    top = functools.reduce(jnp.maximum, maxima)
    scales = [jnp.exp(m - top) for m in maxima]
    total = sum(stat_in[k][:, heads : 2 * heads] * scales[k] for k in range(C))
    inverse = 1.0 / total
    for g in range(heads):
        cols = slice(g * HEAD_SIZE, (g + 1) * HEAD_SIZE)
        mixed = sum(mix_in[k, :, cols].astype(f32) * scales[k][:, g : g + 1] for k in range(C))
        att[c, :, cols] = (mixed * inverse[:, g : g + 1]).astype(bf16)

    for d in range(1, C):
        peer = (c + d) % C
        send(att.at[c], att.at[c], att_s.at[d], att_r.at[c], peer, h)
    loads[0].wait()
    for d in range(1, C):
        peer = (c + C - d) % C
        remote(att.at[peer], att.at[peer], att_s.at[d], att_r.at[peer], peer, h).wait_recv()
    projected = jnp.dot(flat(att[...], rows), ow[...], preferred_element_type=f32)
    po[...] = projected.reshape(H, head_rows, width).astype(bf16)

    for d in range(1, H):
        peer = (h + d) % H
        send(po.at[peer], po_in.at[h], po_s.at[d], po_r.at[h], c, peer)
    po_in[h] = po[h]
    for d in range(1, H):
        peer = (h + H - d) % H
        remote(po_in.at[peer], po_in.at[peer], po_s.at[d], po_r.at[peer], c, peer).wait_recv()
    projected = sum(po_in[k].astype(f32) for k in range(H))
    stream = (res_ref[...].astype(f32) + projected).astype(bf16).astype(f32)
    st_out[...] = stream.reshape(rb, R, width).astype(bf16)
    u_out[...] = (stream * gain_ref[...]).reshape(rb, R, width).astype(bf16)
    squares = jnp.sum(stream * stream, axis=1, keepdims=True)
    ss[c] = jnp.broadcast_to(squares, (head_rows, 128))

    block_head = c // bph
    block_part = c % bph
    u_dst = ublk.at[block_part, pl.ds(h * rb, rb)]
    kept = []
    for d in range(C):
        peer = (c + d) % C
        copy = remote(u_out, u_dst, u_s.at[d], u_r.at[block_part, h], peer, block_head)
        if d == 0:
            kept.append((block_head != h, copy))
            pl.when(block_head != h)(copy.start)

            @pl.when(block_head == h)
            def _():
                ublk[block_part, pl.ds(h * rb, rb)] = u_out[...]

        else:
            copy.start()
            sent.append(copy)
    for d in range(1, C):
        peer = (c + d) % C
        send(ss.at[c], ss.at[c], ss_s.at[d], ss_r.at[c], peer, h)
    for i in range(rb):
        owner = h * rb + i
        other = jnp.logical_or(owner != c, block_head != h)
        copy = remote(
            st_out.at[i], own_st.at[block_part], st_s.at[i], st_r.at[block_part], owner, block_head
        )
        kept.append((other, copy))
        pl.when(other)(copy.start)

        @pl.when(jnp.logical_not(other))
        def _(i=i):
            own_st[block_part] = st_out[i]

    for j in range(bph):
        for k in range(H):
            source = h * bph + j
            block = ublk.at[j, pl.ds(k * rb, rb)]
            arrival = remote(block, block, u_s.at[0], u_r.at[j, k], source, k)
            pl.when(jnp.logical_or(source != c, h != k))(arrival.wait_recv)
    loads[1].wait()
    loads[2].wait()

    def matmul(i, which, weight):
        cols = slice(i * tile, (i + 1) * tile)
        value = None
        for j in range(bph):
            term = jnp.dot(
                flat(ublk[j], rows),
                weight[j * width : (j + 1) * width, cols],
                preferred_element_type=f32,
            )
            value = term if value is None else value + term
        first[i, which] = value.reshape(Y, CORES, head_rows, tile).swapaxes(0, 1).astype(bf16)
        send(
            first.at[i, which, CORES - 1 - core],
            first_in.at[i, which],
            f_s.at[i, which],
            f_r.at[i, which],
            c,
            partner,
        )

    def middle(i, which):
        remote(
            first_in.at[i, which], first_in.at[i, which], f_s.at[i, which], f_r.at[i, which], c, partner
        ).wait_recv()
        both = first[i, which, core].astype(f32) + first_in[i, which].astype(f32)
        second[i, which] = both.astype(bf16)
        for d in range(1, Y):
            peer = (y + d) % Y
            send(
                second.at[i, which, peer],
                second_in.at[i, which, y],
                g_s.at[i, which, d],
                g_r.at[i, which, y],
                c,
                peer * CORES + core,
            )

    def finish(i, inverse_rms):
        sums = []
        for which in range(2):
            value = second[i, which, y].astype(f32)
            for d in range(1, Y):
                peer = (y + Y - d) % Y
                slot = second_in.at[i, which, peer]
                remote(
                    slot, slot, g_s.at[i, which, d], g_r.at[i, which, peer], c, peer * CORES + core
                ).wait_recv()
                value = value + second_in[i, which, peer].astype(f32)
            sums.append(value * inverse_rms)
        hid[i, h] = (jax.nn.gelu(sums[0], approximate=True) * sums[1]).astype(bf16)
        send(hid.at[i, h], hid.at[i, h], h_s.at[i, 0], h_r.at[i, h], c, partner)
        for d in range(1, Y):
            peer = ((y + d) % Y) * CORES + core
            send(hid.at[i, h], hid.at[i, h], h_s.at[i, d], h_r.at[i, h], c, peer)

    def forward(i):
        for d in range(1, Y):
            origin = ((y + Y - d) % Y) * CORES + core
            slot = hid.at[i, origin]
            remote(slot, slot, h_s.at[i, d], h_r.at[i, origin], c, origin).wait_recv()
            send(slot, slot, fw_s.at[i, d], h_r.at[i, origin], c, partner)

    def down(i):
        for d in range(Y):
            origin = ((y + Y - d) % Y) * CORES + (CORES - 1 - core)
            slot = hid.at[i, origin]
            remote(slot, slot, h_s.at[i, 0], h_r.at[i, origin], c, partner).wait_recv()
        term = jnp.dot(
            flat(hid[i], rows), dw[i * tile : (i + 1) * tile, :], preferred_element_type=f32
        )
        if i == 0:
            acc[...] = term
        else:
            acc[...] += term

    steps = [(i, which) for i in range(tiles) for which in range(2)]
    for n, (i, which) in enumerate(steps):
        matmul(i, which, (gw, uw)[which])
        if n:
            middle(*steps[n - 1])
    middle(*steps[-1])
    for d in range(1, C):
        peer = (c + C - d) % C
        remote(ss.at[peer], ss.at[peer], ss_s.at[d], ss_r.at[peer], peer, h).wait_recv()
    squares = sum(ss[k] for k in range(C))
    inverse_rms = lax.rsqrt(squares[:, :1] / (C * width) + norm_epsilon)
    loads[3].wait()
    for i in range(tiles):
        finish(i, inverse_rms)
        if i:
            forward(i - 1)
    forward(tiles - 1)
    for i in range(tiles):
        down(i)
    part[...] = acc[...].reshape(C, R, acc.shape[1]).astype(bf16)

    for d in range(1, C):
        peer = (c + d) % C
        send(part.at[peer], part_in.at[c], part_s.at[d], part_r.at[c], peer, h)
    part_in[c] = part[c]
    for j in range(bph):
        source = h * bph + j
        arrival = remote(own_st.at[j], own_st.at[j], st_s.at[0], st_r.at[j], source, c // rb)
        pl.when(jnp.logical_or(source != c, c // rb != h))(arrival.wait_recv)
    own_ref[...] = own_st[...]
    for d in range(1, C):
        peer = (c + C - d) % C
        remote(part_in.at[peer], part_in.at[peer], part_s.at[d], part_r.at[peer], peer, h).wait_recv()
    mlp_ref[...] = sum(part_in[k].astype(f32) for k in range(C))
    for copy in sent:
        copy.wait_send()
    for condition, copy in kept:
        pl.when(condition)(copy.wait_send)


def tail(C, H, mixture, stats, residual_in, norm_gain, out_weight, gate_weight, up_weight, down_weight):
    rows, query_width = mixture.shape
    R = rows // C
    width = out_weight.shape[1]
    hidden = gate_weight.shape[1]
    out_width = down_weight.shape[1]
    rb = C // H
    bph = C // H
    Y = H // CORES
    head_rows = rows // H
    tile = column_tile(hidden)
    tiles = hidden // tile
    bf16 = jnp.bfloat16
    vmem = pl.BlockSpec(memory_space=pltpu.VMEM)
    hbm = pl.BlockSpec(memory_space=pl.ANY)
    V = pltpu.VMEM
    S = pltpu.SemaphoreType.DMA
    return pl.pallas_call(
        functools.partial(tail_kernel, C, H),
        out_shape=(
            jax.ShapeDtypeStruct((R, out_width), jnp.float32),
            jax.ShapeDtypeStruct((bph, R, width), bf16),
        ),
        in_specs=[vmem] * 4 + [hbm] * 4,
        out_specs=(vmem, vmem),
        scratch_shapes=[
            V(out_weight.shape, bf16),
            V(gate_weight.shape, bf16),
            V(up_weight.shape, bf16),
            V(down_weight.shape, bf16),
            V((C, R, query_width), bf16),
            V((C, R, 128), jnp.float32),
            V((C, R, query_width), bf16),
            V((H, head_rows, width), bf16),
            V((H, head_rows, width), bf16),
            V((rb, R, width), bf16),
            V((rb, R, width), bf16),
            V((C, head_rows, 128), jnp.float32),
            V((bph, C, R, width), bf16),
            V((bph, R, width), bf16),
            V((tiles, 2, CORES, Y, head_rows, tile), bf16),
            V((tiles, 2, Y, head_rows, tile), bf16),
            V((tiles, 2, Y, head_rows, tile), bf16),
            V((tiles, 2, Y, head_rows, tile), bf16),
            V((tiles, H, head_rows, tile), bf16),
            V((rows, out_width), jnp.float32),
            V((C, R, out_width), bf16),
            V((C, R, out_width), bf16),
            S((4,)),
            S((C,)),
            S((C,)),
            S((C,)),
            S((C,)),
            S((C,)),
            S((C,)),
            S((H,)),
            S((H,)),
            S((C,)),
            S((bph, H)),
            S((rb,)),
            S((bph,)),
            S((C,)),
            S((C,)),
            S((tiles, 2)),
            S((tiles, 2)),
            S((tiles, 2, Y)),
            S((tiles, 2, Y)),
            S((tiles, Y)),
            S((tiles, H)),
            S((tiles, Y)),
            S((C,)),
            S((C,)),
        ],
        compiler_params=pltpu.CompilerParams(
            has_side_effects=True, vmem_limit_bytes=60 * 2**20
        ),
    )(
        mixture.reshape(C, R, query_width),
        stats.reshape(C, R, 128),
        residual_in,
        norm_gain.reshape(1, width),
        out_weight,
        gate_weight,
        up_weight,
        down_weight,
    )


def shards(
    queries,
    keys,
    values,
    page_map,
    selected,
    residual_in,
    out_weight,
    norm_gain,
    gate_weight,
    up_weight,
    down_weight,
):
    ctx_index = lax.axis_index("ctx")
    C = lax.axis_size("ctx")
    H = lax.axis_size("head")
    row_max, row_total, mixture = owner_pass(
        queries, keys, values, page_map, selected, ctx_index, C
    )
    stats = jnp.concatenate([row_max, row_total], axis=1)
    stats = jnp.pad(stats, ((0, 0), (0, 128 - stats.shape[1])))
    mlp_out, own_stream = tail(
        C,
        H,
        mixture.astype(jnp.bfloat16),
        stats,
        residual_in,
        norm_gain,
        out_weight,
        gate_weight,
        up_weight,
        down_weight,
    )
    own_stream = jnp.concatenate([own_stream[j] for j in range(own_stream.shape[0])], axis=1)
    return (own_stream.astype(jnp.float32) + mlp_out).astype(jnp.bfloat16)


def solution(mesh):
    in_specs = (
        P(None, "head"),
        P("ctx", None, "head"),
        P("ctx", None, "head"),
        P(),
        P(),
        P("head", "ctx"),
        P("head", "ctx"),
        P("ctx"),
        P("head", "ctx"),
        P("head", "ctx"),
        P("ctx", "head"),
    )
    out_specs = P("ctx", "head")
    return jax.shard_map(shards, mesh=mesh, in_specs=in_specs, out_specs=out_specs, check_vma=False)
```
